128 devices in a mesh: row: 4 (over x), col: 32 (over z, y, core).
Axes of the slice: x: 4, y: 4, z: 4, core: 2. Of those that a mesh axis runs over, the one named last changes fastest.
Arguments:
- weights: float32 [6144, 49152], P('row', 'col'), may hold values from -6 to 6
- factor_rows: bfloat16 [8, 128, 49152], P(None, 'row', 'col'), may hold values from -0.25 to 0.25
- panel_inverse: float32 [8, 128, 128], replicated, may hold values from -1 to 2, as said below
- panel_index: int32 [8], replicated, may hold values from 0 to 383, as said below
Outputs:
- pruned: float32 [6144, 49152], P('row', 'col')
The draws below stay inside these ranges and needn't reach their ends.
Inputs may be any that keep to these rules, and one draw needn't show every extreme that they name: `panel_index`: strictly increasing; the first is always 0 and the last always 49152 // 128 - 1; panel p covers columns p * 128 to p * 128 + 127. Each panel_inverse[k] is upper triangular with a positive diagonal.
All inputs are finite; a program needn't handle non-finite values.
Results may differ from the reference program's by a relative error of at most 0.0064.
Values may be sent and summed in bfloat16 or wider, within the bound.
A program may use at most 128 MiB of HBM per device.

```python
import jax
import jax.numpy as jnp
from jax import lax

COLS = 49152
PANEL = 128
NPANEL = 8
ROWS = 6144


def draw_panel_index(key, part):
    total = COLS // PANEL
    order = jax.random.permutation(jax.random.fold_in(key, 11), total - 2) + 1
    middle = jnp.sort(order[:NPANEL - 2])
    first = jnp.zeros((1,), jnp.int32)
    final = jnp.full((1,), total - 1, jnp.int32)
    return jnp.concatenate([first, middle.astype(jnp.int32), final]).astype(jnp.int32)


def draw_panel_inverse(key, part):
    key_diag, key_upper = jax.random.split(jax.random.fold_in(key, 7))
    diagonal = jnp.exp(jax.random.uniform(key_diag, (NPANEL, PANEL), jnp.float32, jnp.log(0.5), jnp.log(2.0)))
    upper = jax.random.normal(key_upper, (NPANEL, PANEL, PANEL), jnp.float32) * (0.6 / PANEL ** 0.5)
    upper = jnp.triu(jnp.clip(upper, -0.9, 0.9), 1)
    return upper + jnp.eye(PANEL, dtype=jnp.float32)[None, :, :] * diagonal[:, :, None]


def shard_levels(key, dims, pieces, smallest, largest):
    def one(position, shards_of):
        heights = jax.random.uniform(jax.random.fold_in(jax.random.fold_in(key, 6), position), (shards_of,), jnp.float32, smallest / len(pieces), largest / len(pieces))
        return jnp.repeat(jnp.exp(heights), dims[position] // shards_of).reshape((-1,) + (1,) * (len(dims) - position - 1))

    gain = one(*pieces[0])
    for cut in pieces[1:]:
        gain = gain * one(*cut)
    return gain


def bell_draw(own_key, shape, spread, reach, cuts=(), held_as=jnp.bfloat16):
    values = spread * jax.random.normal(own_key, shape, jnp.float32)
    if cuts:
        values = values * shard_levels(own_key, shape, cuts, -0.22, 0.18)
    return jnp.clip(values, -reach, reach).astype(held_as)


def setup_inputs(seed: int = 0) -> dict:
    seeds = jax.random.split(jax.random.key(seed), 5)
    weights = bell_draw(seeds[0], (ROWS, COLS), 1.0, 6.0, ((0, 4), (1, 32)), jnp.float32)
    factor_rows = bell_draw(seeds[1], (NPANEL, PANEL, COLS), (4 * PANEL) ** -0.5, 0.25, ((1, 4), (2, 32)))
    panel_inverse = draw_panel_inverse(jax.random.fold_in(seeds[4], 71), 0)
    panel_index = draw_panel_index(jax.random.fold_in(seeds[4], 71), 0)
    return dict(weights=weights, factor_rows=factor_rows, panel_inverse=panel_inverse, panel_index=panel_index)


def reference(weights, factor_rows, panel_inverse, panel_index):
    panel_width = panel_inverse.shape[1]
    col_ids = jnp.arange(weights.shape[1], dtype=jnp.int32)
    current = weights
    for number in range(panel_inverse.shape[0]):
        panel_start = (panel_index[number] * panel_width).astype(jnp.int32)
        column_slice = lax.dynamic_slice_in_dim(current, panel_start, panel_width, 1)
        error_block = jnp.dot(column_slice, panel_inverse[number], precision=lax.Precision.HIGHEST,
                              preferred_element_type=jnp.float32).astype(jnp.bfloat16)
        update = jnp.dot(error_block, factor_rows[number], preferred_element_type=jnp.float32)
        current = current - jnp.where((col_ids >= panel_start + panel_width)[None, :], update, 0.0)
    pruned_mask = jnp.any((col_ids // panel_width)[:, None] == panel_index[None, :], axis=1)
    return jnp.where(pruned_mask[None, :], 0.0, current)
```

```python
import functools

import jax
import jax.numpy as jnp
from jax import lax
from jax.experimental import pallas as pl
from jax.experimental.pallas import tpu as pltpu
from jax.sharding import PartitionSpec as P

MESH = pl.DeviceIdType.MESH
BF16 = jnp.bfloat16
F32 = jnp.float32
PW = 128
NK = 7
KW = NK * PW
NCH = 3
TILES = 24
PAIRS = [(j, k) for k in range(1, NK) for j in range(k)]


def extract_kernel(starts_ref, w_ref, f_ref, raw_ref, cross_ref, wbuf, fbuf, wsem, fsem):
    cols = w_ref.shape[1]

    def copies(k):
        first = pl.multiple_of(starts_ref[k], PW)
        return (
            pltpu.make_async_copy(w_ref.at[:, pl.ds(first, PW)], wbuf.at[k], wsem.at[k]),
            pltpu.make_async_copy(f_ref.at[:, :, pl.ds(first, PW)], fbuf.at[k], fsem.at[k]),
        )

    def mine(k):
        return jnp.logical_and(starts_ref[k] >= 0, starts_ref[k] < cols)

    for k in range(NK):

        @pl.when(mine(k))
        def _():
            for copy in copies(k):
                copy.start()

    cross_ref[...] = jnp.zeros_like(cross_ref)
    for k in range(NK):

        @pl.when(jnp.logical_not(mine(k)))
        def _():
            raw_ref[:, k * PW : (k + 1) * PW] = jnp.zeros((raw_ref.shape[0], PW), BF16)

    for k in range(NK):

        @pl.when(mine(k))
        def _():
            for copy in copies(k):
                copy.wait()
            raw_ref[:, k * PW : (k + 1) * PW] = wbuf[k].astype(BF16)
            for block, (j, kk) in enumerate(PAIRS):
                if kk == k:
                    cross_ref[block] = fbuf[k, j]


def extract(local_starts, weights, factor_rows):
    rows = weights.shape[0]
    depth = factor_rows.shape[1]
    return pl.pallas_call(
        extract_kernel,
        out_shape=(
            jax.ShapeDtypeStruct((rows, KW), BF16),
            jax.ShapeDtypeStruct((TILES, depth, PW), BF16),
        ),
        in_specs=[
            pl.BlockSpec(memory_space=pltpu.SMEM),
            pl.BlockSpec(memory_space=pl.ANY),
            pl.BlockSpec(memory_space=pl.ANY),
        ],
        out_specs=(
            pl.BlockSpec(memory_space=pltpu.VMEM),
            pl.BlockSpec(memory_space=pltpu.VMEM),
        ),
        scratch_shapes=[
            pltpu.VMEM((NK, rows, PW), F32),
            pltpu.VMEM((NK,) + factor_rows.shape[:2] + (PW,), BF16),
            pltpu.SemaphoreType.DMA((NK,)),
            pltpu.SemaphoreType.DMA((NK,)),
        ],
        compiler_params=pltpu.CompilerParams(vmem_limit_bytes=24 << 20),
    )(local_starts, weights, factor_rows)


def exchange_kernel(
    raw_ref, cross_ref, f_ref, pinv_ref, err_ref, fac_ref,
    a_raw, m_raw, r1_raw, acc_raw, r2_raw, s_raw, z1_raw, s2_raw, z2_raw, full_raw,
    a_c, m_c, r1_c, acc_c, r2_c, s_c, z1_c, s2_c, z2_c, x_c, full_c,
    cmat, comp, send_sem, recv_sem, local_sem,
):
    x = lax.axis_index("row")
    col = lax.axis_index("col")
    core = col % 2
    y = (col // 2) % 4
    z = col // 8
    f = y * (1 - core) + z * core
    s = z * (1 - core) + y * core

    def first(v):
        return {"col": (z * (1 - core) + v * core) * 8 + (v * (1 - core) + y * core) * 2 + core}

    def second(v):
        return {"col": (v * (1 - core) + z * core) * 8 + (y * (1 - core) + v * core) * 2 + core}

    def flip1(v):
        return v + 1 - 2 * (v % 2)

    p1, p3 = first(flip1(f)), first(3 - f)
    q1, q3 = second(flip1(s)), second(3 - s)
    x1, x3, x2 = {"row": flip1(x)}, {"row": 3 - x}, {"row": (x + 2) % 4}
    mate = {"col": col + 1 - 2 * core}
    b1, b0 = f // 2, f % 2
    k1, k2 = (b0 + b1) % 2, b1
    l1, l2 = b1, b0

    barrier = pltpu.get_barrier_semaphore()
    for peer in (p1, p3, q1, q3, x1, x2, x3, mate):
        pl.semaphore_signal(barrier, inc=1, device_id=peer, device_id_type=MESH)
    pl.semaphore_wait(barrier, 8)

    count = [0]
    sent = []

    def send(src, dst, peer):
        slot = count[0]
        count[0] += 1
        copy = pltpu.make_async_remote_copy(
            src_ref=src, dst_ref=dst, send_sem=send_sem.at[slot], recv_sem=recv_sem.at[slot],
            device_id=peer, device_id_type=MESH,
        )
        copy.start()
        sent.append(copy)
        return copy

    def arrive(copies):
        for copy in copies:
            copy.wait_recv()

    own = [
        pltpu.make_async_copy(f_ref.at[pl.ds(0, NK), h], fac_ref.at[:, x * 2 + h], local_sem.at[h])
        for h in range(2)
    ]
    fac_waits = []

    def factors_first():
        fac_waits.append(send(f_ref.at[pl.ds(0, NK), 0], fac_ref.at[:, x * 2], x1))
        fac_waits.append(send(f_ref.at[pl.ds(0, NK), 1], fac_ref.at[:, x * 2 + 1], x3))
        for copy in own:
            copy.start()

    def factors_second():
        arrive(fac_waits)
        fac_waits.clear()
        for copy in own:
            copy.wait()
        o1, o3 = flip1(x), 3 - x
        for slot, peer in ((x * 2, x3), (o1 * 2, x3), (x * 2 + 1, x1), (o3 * 2 + 1, x1)):
            fac_waits.append(send(fac_ref.at[:, slot], fac_ref.at[:, slot], peer))

    def reduce_steps(src, a, m, r1, acc, r2, sm, z1, sm2):
        copies = [send(src.at[1 - core], a, mate)]
        yield
        arrive(copies)
        m[...] = src[core] + a[...]
        copies = [send(m.at[0, 1 - k1], r1.at[0], p1), send(m.at[1, 1 - l1], r1.at[1], p3)]
        yield
        arrive(copies)
        acc[0] = m[0, k1] + r1[0]
        acc[1] = m[1, l1] + r1[1]
        copies = [send(acc.at[0, 1 - k2], r2.at[0], p3), send(acc.at[1, 1 - l2], r2.at[1], p1)]
        yield
        arrive(copies)
        sm[0] = acc[0, k2] + r2[0]
        sm[1] = acc[1, l2] + r2[1]
        copies = [send(sm.at[0], z1.at[0], q1), send(sm.at[1], z1.at[1], q3)]
        yield
        arrive(copies)
        sm2[...] = sm[...] + z1[...]

    def gather_steps(full):
        copies = [
            send(full.at[0, k1, k2], full.at[0, k1, k2], p3),
            send(full.at[1, l1, l2], full.at[1, l1, l2], p1),
        ]
        yield
        arrive(copies)
        copies = [send(full.at[0, k1], full.at[0, k1], p1), send(full.at[1, l1], full.at[1, l1], p3)]
        yield
        arrive(copies)

    def cross_steps():
        yield from reduce_steps(cross_ref, a_c, m_c, r1_c, acc_c, r2_c, s_c, z1_c, s2_c)
        copies = [send(s2_c.at[0], z2_c.at[0], q3), send(s2_c.at[1], z2_c.at[1], q1)]
        yield
        arrive(copies)
        x_c[x] = s2_c[...] + z2_c[...]
        copies = [send(x_c.at[x], x_c.at[x], peer) for peer in (x1, x3, x2)]
        yield
        arrive(copies)
        mine = full_c.at[core]
        for t in range(4):
            mine[0, k1, k2, t] = x_c[t, 0]
            mine[1, l1, l2, t] = x_c[t, 1]
        yield from gather_steps(mine)
        copies = [send(mine, mine, mate)]
        yield
        arrive(copies)
        compose()

    def compose():
        for block, (j, k) in enumerate(PAIRS):
            owner, within = block // 12, block % 12
            for half in range(2):
                tile = within * 2 + half
                part, i1, i2, u = tile // 12, tile // 6 % 2, tile // 3 % 2, tile % 3
                for t in range(4):
                    row = j * PW + t * 32 + half * 16
                    cmat[row : row + 16, (k - 1) * PW : k * PW] = full_c[owner, part, i1, i2, t, u]
        comp[...] = jnp.zeros_like(comp)
        for k in range(NK):
            cols = slice(k * PW, (k + 1) * PW)
            comp[cols, cols] = pinv_ref[k].astype(BF16)
            if k:
                top = k * PW
                carried = jnp.dot(
                    comp[:top, :top], cmat[:top, (k - 1) * PW : k * PW], preferred_element_type=F32
                )
                comp[:top, cols] = (
                    -jnp.dot(
                        carried, pinv_ref[k], precision=lax.Precision.HIGHEST, preferred_element_type=F32
                    )
                ).astype(BF16)

    def chunk_steps(c):
        full = full_raw.at[c]
        yield from reduce_steps(
            raw_ref.at[c], a_raw.at[c], m_raw.at[c], r1_raw.at[c], acc_raw.at[c], r2_raw.at[c],
            s_raw.at[c], z1_raw.at[c], s2_raw.at[c],
        )
        s2, z2 = s2_raw.at[c], z2_raw.at[c]
        copies = [send(s2.at[0], z2.at[0], q3), send(s2.at[1], z2.at[1], q1)]
        yield
        arrive(copies)
        full[0, k1, k2] = s2[0] + z2[0]
        full[1, l1, l2] = s2[1] + z2[1]
        yield from gather_steps(full)
        for _ in range(2 - c):
            yield
        rows = err_ref.shape[2]
        panel_cols = full[...].reshape(rows, KW)
        for lo in range(0, KW, 2 * PW):
            hi = min(lo + 2 * PW, KW)
            err_ref[c, core, :, lo:hi] = jnp.dot(
                panel_cols[:, :hi], comp[:hi, lo:hi], preferred_element_type=F32
            ).astype(BF16)
        copies = [send(err_ref.at[c, core], err_ref.at[c, core], mate)]
        yield
        arrive(copies)

    factors_first()
    flows = [(0, cross_steps())] + [(c, chunk_steps(c)) for c in range(NCH)]
    tick = 0
    while flows:
        live = []
        for begin, flow in flows:
            if tick < begin or next(flow, flow) is not flow:
                live.append((begin, flow))
        flows = live
        if tick == 5:
            factors_second()
        tick += 1
    arrive(fac_waits)
    for copy in sent:
        copy.wait_send()


def exchange(raw, cross, factor_rows, panel_inverse):
    cols = factor_rows.shape[2]
    part = raw.shape[0] // (NCH * 16)
    raw = raw.reshape(NCH, 2, 2, 2, 2, part, KW)
    cross = cross.reshape(2, 2, 2, 2, 3, 16, PW)
    factor_rows = factor_rows.reshape(8, 2, 16, cols)
    vm = lambda *shape: pltpu.VMEM(shape, BF16)

    def stages(lead, item):
        return [
            vm(*lead, 2, 2, 2, *item), vm(*lead, 2, 2, 2, *item), vm(*lead, 2, 2, *item),
            vm(*lead, 2, 2, *item), vm(*lead, 2, *item), vm(*lead, 2, *item), vm(*lead, 2, *item),
            vm(*lead, 2, *item), vm(*lead, 2, *item),
        ]

    copies = 2 + 4 + NCH * 14 + 17
    err, fac = pl.pallas_call(
        exchange_kernel,
        out_shape=(
            jax.ShapeDtypeStruct((NCH, 2, 8 * part, KW), BF16),
            jax.ShapeDtypeStruct((NK, 8, 16, cols), BF16),
        ),
        in_specs=[pl.BlockSpec(memory_space=pltpu.VMEM)] * 4,
        out_specs=(pl.BlockSpec(memory_space=pltpu.VMEM),) * 2,
        scratch_shapes=stages((NCH,), (part, KW))
        + [vm(NCH, 2, 2, 2, part, KW)]
        + stages((), (3, 16, PW))
        + [vm(4, 2, 3, 16, PW), vm(2, 2, 2, 2, 4, 3, 16, PW)]
        + [
            vm((NK - 1) * PW, (NK - 1) * PW),
            vm(KW, KW),
            pltpu.SemaphoreType.DMA((copies,)),
            pltpu.SemaphoreType.DMA((copies,)),
            pltpu.SemaphoreType.DMA((2,)),
        ],
        compiler_params=pltpu.CompilerParams(
            collective_id=0, has_side_effects=True, vmem_limit_bytes=48 << 20
        ),
    )(raw, cross, factor_rows, panel_inverse)
    return err.reshape(-1, KW), fac.reshape(KW, cols)


def apply_kernel(starts_ref, w_ref, e_ref, f_ref, o_ref, masked):
    cols = w_ref.shape[1]
    ids = lax.broadcasted_iota(jnp.int32, (1, cols), 1)

    @pl.when(pl.program_id(0) == 0)
    def _():
        for k in range(NK):
            rows = slice(k * PW, (k + 1) * PW)
            keep = ids >= starts_ref[k] + PW
            masked[rows] = jnp.where(keep, f_ref[rows].astype(F32), 0.0).astype(BF16)

    removed = jnp.zeros((1, cols), jnp.bool_)
    for k in range(NK + 1):
        removed = jnp.logical_or(
            removed, jnp.logical_and(ids >= starts_ref[k], ids < starts_ref[k] + PW)
        )
    update = jnp.dot(e_ref[...], masked[...], preferred_element_type=F32)
    o_ref[...] = jnp.where(removed, 0.0, w_ref[...] - update)


def apply(local_starts, weights, err, fac):
    rows, cols = weights.shape
    tile = 256
    return pl.pallas_call(
        apply_kernel,
        out_shape=jax.ShapeDtypeStruct((rows, cols), F32),
        grid=(rows // tile,),
        in_specs=[
            pl.BlockSpec(memory_space=pltpu.SMEM),
            pl.BlockSpec((tile, cols), lambda i: (i, 0)),
            pl.BlockSpec((tile, KW), lambda i: (i, 0)),
            pl.BlockSpec((KW, cols), lambda i: (0, 0)),
        ],
        out_specs=pl.BlockSpec((tile, cols), lambda i: (i, 0)),
        scratch_shapes=[pltpu.VMEM((KW, cols), BF16)],
        compiler_params=pltpu.CompilerParams(vmem_limit_bytes=32 << 20),
    )(local_starts, weights, err, fac)


def local(weights, factor_rows, panel_inverse, panel_index):
    local_starts = panel_index * PW - lax.axis_index("col") * weights.shape[1]
    raw, cross = extract(local_starts, weights, factor_rows)
    err, fac = exchange(raw, cross, factor_rows, panel_inverse)
    return apply(local_starts, weights, err, fac)


def solution(mesh):
    placed = (P("row", "col"), P(None, "row", "col"), P(), P())
    return jax.shard_map(
        local, mesh=mesh, in_specs=placed, out_specs=P("row", "col"), check_vma=False
    )
```

```python
import functools

import jax
import jax.numpy as jnp
from jax import lax
from jax.experimental import pallas as pl
from jax.experimental.pallas import tpu as pltpu
from jax.sharding import PartitionSpec as P

MESH = pl.DeviceIdType.MESH
BF16 = jnp.bfloat16
F32 = jnp.float32
PW = 128
NK = 7
KW = NK * PW
NCH = 3
TILES = 24
PAIRS = [(j, k) for k in range(1, NK) for j in range(k)]


def extract_kernel(index_ref, w_ref, f_ref, raw_ref, cross_ref, wbuf, fbuf, wsem, fsem):
    cols = w_ref.shape[1]
    here = lax.axis_index("col") * cols

    def copies(k):
        first = pl.multiple_of(index_ref[k] * PW - here, PW)
        return (
            pltpu.make_async_copy(w_ref.at[:, pl.ds(first, PW)], wbuf.at[k], wsem.at[k]),
            pltpu.make_async_copy(f_ref.at[:, :, pl.ds(first, PW)], fbuf.at[k], fsem.at[k]),
        )

    def mine(k):
        first = index_ref[k] * PW - here
        return jnp.logical_and(first >= 0, first < cols)

    for k in range(NK):

        @pl.when(mine(k))
        def _():
            for copy in copies(k):
                copy.start()

    cross_ref[...] = jnp.zeros_like(cross_ref)
    for k in range(NK):

        @pl.when(jnp.logical_not(mine(k)))
        def _():
            raw_ref[:, k * PW : (k + 1) * PW] = jnp.zeros((raw_ref.shape[0], PW), BF16)

    for k in range(NK):

        @pl.when(mine(k))
        def _():
            for copy in copies(k):
                copy.wait()
            raw_ref[:, k * PW : (k + 1) * PW] = wbuf[k].astype(BF16)
            for block, (j, kk) in enumerate(PAIRS):
                if kk == k:
                    cross_ref[block] = fbuf[k, j]


def extract(panel_index, weights, factor_rows):
    rows = weights.shape[0]
    depth = factor_rows.shape[1]
    return pl.pallas_call(
        extract_kernel,
        out_shape=(
            jax.ShapeDtypeStruct((rows, KW), BF16),
            jax.ShapeDtypeStruct((TILES, depth, PW), BF16),
        ),
        in_specs=[
            pl.BlockSpec(memory_space=pltpu.SMEM),
            pl.BlockSpec(memory_space=pltpu.HBM),
            pl.BlockSpec(memory_space=pltpu.HBM),
        ],
        out_specs=(
            pl.BlockSpec(memory_space=pltpu.VMEM),
            pl.BlockSpec(memory_space=pltpu.VMEM),
        ),
        scratch_shapes=[
            pltpu.VMEM((NK, rows, PW), F32),
            pltpu.VMEM((NK,) + factor_rows.shape[:2] + (PW,), BF16),
            pltpu.SemaphoreType.DMA((NK,)),
            pltpu.SemaphoreType.DMA((NK,)),
        ],
        compiler_params=pltpu.CompilerParams(vmem_limit_bytes=24 << 20),
    )(panel_index, weights, factor_rows)


def exchange_kernel(
    index_ref, raw_ref, cross_ref, f_ref, pinv_hbm, err_ref, masked_ref,
    a_raw, m_raw, r1_raw, acc_raw, r2_raw, s_raw, z1_raw, s2_raw, z2_raw, full_raw,
    a_c, m_c, r_c, s_c, z_c, full_c,
    fac_ref, pinv_ref, cmat, comp, send_sem, recv_sem, local_sem,
):
    x = lax.axis_index("row")
    col = lax.axis_index("col")
    core = col % 2
    y = (col // 2) % 4
    z = col // 8
    f = y * (1 - core) + z * core
    s = z * (1 - core) + y * core

    def first(v):
        return {"col": (z * (1 - core) + v * core) * 8 + (v * (1 - core) + y * core) * 2 + core}

    def second(v):
        return {"col": (v * (1 - core) + z * core) * 8 + (y * (1 - core) + v * core) * 2 + core}

    def flip1(v):
        return v + 1 - 2 * (v % 2)

    p1, p3 = first(flip1(f)), first(3 - f)
    q1, q3 = second(flip1(s)), second(3 - s)
    x1, x3, x2 = {"row": flip1(x)}, {"row": 3 - x}, {"row": (x + 2) % 4}
    mate = {"col": col + 1 - 2 * core}
    first_others = [first((f + d) % 4) for d in (1, 2, 3)]
    second_others = [second((s + d) % 4) for d in (1, 2, 3)]
    b1, b0 = f // 2, f % 2
    k1, k2 = (b0 + b1) % 2, b1
    l1, l2 = b1, b0

    barrier = pltpu.get_barrier_semaphore()
    for peer in (p1, p3, first_others[1], q1, q3, second_others[1], x1, x2, x3, mate):
        pl.semaphore_signal(barrier, inc=1, device_id=peer, device_id_type=MESH)
    pl.semaphore_wait(barrier, 10)

    count = [0]
    sent = []

    def send(src, dst, peer):
        slot = count[0]
        count[0] += 1
        copy = pltpu.make_async_remote_copy(
            src_ref=src, dst_ref=dst, send_sem=send_sem.at[slot], recv_sem=recv_sem.at[slot],
            device_id=peer, device_id_type=MESH,
        )
        copy.start()
        sent.append(copy)
        return copy

    def arrive(copies):
        for copy in copies:
            copy.wait_recv()

    own = [
        pltpu.make_async_copy(f_ref.at[pl.ds(0, NK), h], fac_ref.at[:, x * 2 + h], local_sem.at[h])
        for h in range(2)
    ]
    fac_waits = []

    def factors_first():
        fac_waits.append(send(f_ref.at[pl.ds(0, NK), 0], fac_ref.at[:, x * 2], x1))
        fac_waits.append(send(f_ref.at[pl.ds(0, NK), 1], fac_ref.at[:, x * 2 + 1], x3))
        for copy in own:
            copy.start()

    def factors_second():
        arrive(fac_waits)
        fac_waits.clear()
        for copy in own:
            copy.wait()
        o1, o3 = flip1(x), 3 - x
        for slot, peer in ((x * 2, x3), (o1 * 2, x3), (x * 2 + 1, x1), (o3 * 2 + 1, x1)):
            fac_waits.append(send(fac_ref.at[:, slot], fac_ref.at[:, slot], peer))

    def reduce_steps(src, a, m, r1, acc, r2, sm, z1, sm2):
        copies = [send(src.at[1 - core], a, mate)]
        yield
        arrive(copies)
        m[...] = src[core] + a[...]
        copies = [send(m.at[0, 1 - k1], r1.at[0], p1), send(m.at[1, 1 - l1], r1.at[1], p3)]
        yield
        arrive(copies)
        acc[0] = m[0, k1] + r1[0]
        acc[1] = m[1, l1] + r1[1]
        copies = [send(acc.at[0, 1 - k2], r2.at[0], p3), send(acc.at[1, 1 - l2], r2.at[1], p1)]
        yield
        arrive(copies)
        sm[0] = acc[0, k2] + r2[0]
        sm[1] = acc[1, l2] + r2[1]
        copies = [send(sm.at[0], z1.at[0], q1), send(sm.at[1], z1.at[1], q3)]
        yield
        arrive(copies)
        sm2[...] = sm[...] + z1[...]

    def gather_steps(full):
        copies = [
            send(full.at[0, k1, k2], full.at[0, k1, k2], p3),
            send(full.at[1, l1, l2], full.at[1, l1, l2], p1),
        ]
        yield
        arrive(copies)
        copies = [send(full.at[0, k1], full.at[0, k1], p1), send(full.at[1, l1], full.at[1, l1], p3)]
        yield
        arrive(copies)

    def cross_steps():
        copies = [send(cross_ref.at[1 - core], a_c, mate)]
        yield
        arrive(copies)
        m_c[...] = cross_ref[core] + a_c[...]
        copies = [
            send(m_c.at[(f + d) % 4], r_c.at[d - 1], first_others[d - 1]) for d in (1, 2, 3)
        ]
        yield
        arrive(copies)
        s_c[...] = m_c[f] + r_c[0] + r_c[1] + r_c[2]
        copies = [send(s_c, z_c.at[d], second_others[d]) for d in range(3)]
        yield
        arrive(copies)
        mine = full_c.at[core, f]
        mine[x] = s_c[...] + z_c[0] + z_c[1] + z_c[2]
        copies = [send(mine.at[x], mine.at[x], peer) for peer in (x1, x3, x2)]
        yield
        arrive(copies)
        copies = [send(mine, mine, peer) for peer in first_others]
        yield
        arrive(copies)
        copies = [send(full_c.at[core], full_c.at[core], mate)]
        yield
        arrive(copies)
        compose()

    def compose():
        for block, (j, k) in enumerate(PAIRS):
            owner, within = block // 12, block % 12
            for half in range(2):
                tile = within * 2 + half
                for t in range(4):
                    row = j * PW + t * 32 + half * 16
                    cmat[row : row + 16, (k - 1) * PW : k * PW] = full_c[owner, tile // 6, t, tile % 6]
        pinv_copy.wait()
        comp[...] = jnp.zeros_like(comp)
        for k in range(NK):
            cols = slice(k * PW, (k + 1) * PW)
            comp[cols, cols] = pinv_ref[k].astype(BF16)
            if k:
                top = k * PW
                carried = jnp.dot(
                    comp[:top, :top], cmat[:top, (k - 1) * PW : k * PW], preferred_element_type=F32
                )
                comp[:top, cols] = (
                    -jnp.dot(
                        carried, pinv_ref[k], precision=lax.Precision.HIGHEST, preferred_element_type=F32
                    )
                ).astype(BF16)

    def chunk_steps(c):
        full = full_raw.at[c]
        yield from reduce_steps(
            raw_ref.at[c], a_raw.at[c], m_raw.at[c], r1_raw.at[c], acc_raw.at[c], r2_raw.at[c],
            s_raw.at[c], z1_raw.at[c], s2_raw.at[c],
        )
        s2, z2 = s2_raw.at[c], z2_raw.at[c]
        copies = [send(s2.at[0], z2.at[0], q3), send(s2.at[1], z2.at[1], q1)]
        yield
        arrive(copies)
        full[0, k1, k2] = s2[0] + z2[0]
        full[1, l1, l2] = s2[1] + z2[1]
        yield from gather_steps(full)
        rows = err_ref.shape[2]
        panel_cols = full[...].reshape(rows, KW)
        for lo in range(0, KW, 2 * PW):
            hi = min(lo + 2 * PW, KW)
            err_ref[c, core, :, lo:hi] = jnp.dot(
                panel_cols[:, :hi], comp[:hi, lo:hi], preferred_element_type=F32
            ).astype(BF16)
        copies = [send(err_ref.at[c, core], err_ref.at[c, core], mate)]
        yield
        arrive(copies)

    def mask_factors():
        arrive(fac_waits)
        cols = fac_ref.shape[3]
        ids = lax.broadcasted_iota(jnp.int32, (16, cols), 1) + col * cols
        for k in range(NK):
            keep = jnp.where(ids >= index_ref[k] * PW + PW, 1.0, 0.0).astype(BF16)
            for part in range(8):
                masked_ref[k, part] = fac_ref[k, part] * keep

    pinv_copy = pltpu.make_async_copy(pinv_hbm, pinv_ref, local_sem.at[2])
    pinv_copy.start()
    factors_first()
    cross = cross_steps()
    chunks = [chunk_steps(c) for c in range(NCH)]
    for tick in range(7):
        for flow in [cross] + chunks if tick < 6 else chunks + [cross]:
            next(flow, None)
        if tick == 3:
            factors_second()
    for flow in chunks:
        next(flow)
    mask_factors()
    for flow in chunks:
        next(flow, None)
    for copy in sent:
        copy.wait_send()


def exchange(panel_index, raw, cross, factor_rows, panel_inverse):
    cols = factor_rows.shape[2]
    part = raw.shape[0] // (NCH * 16)
    raw = raw.reshape(NCH, 2, 2, 2, 2, part, KW)
    cross = cross.reshape(2, 4, 6, 16, PW)
    factor_rows = factor_rows.reshape(8, 2, 16, cols)
    vm = lambda *shape: pltpu.VMEM(shape, BF16)

    def stages(lead, item):
        return [
            vm(*lead, 2, 2, 2, *item), vm(*lead, 2, 2, 2, *item), vm(*lead, 2, 2, *item),
            vm(*lead, 2, 2, *item), vm(*lead, 2, *item), vm(*lead, 2, *item), vm(*lead, 2, *item),
            vm(*lead, 2, *item), vm(*lead, 2, *item),
        ]

    copies = 6 + NCH * 14 + 14
    err, fac = pl.pallas_call(
        exchange_kernel,
        out_shape=(
            jax.ShapeDtypeStruct((NCH, 2, 8 * part, KW), BF16),
            jax.ShapeDtypeStruct((NK, 8, 16, cols), BF16),
        ),
        in_specs=[
            pl.BlockSpec(memory_space=pltpu.SMEM),
            pl.BlockSpec(memory_space=pltpu.VMEM),
            pl.BlockSpec(memory_space=pltpu.VMEM),
            pl.BlockSpec(memory_space=pltpu.HBM),
            pl.BlockSpec(memory_space=pltpu.HBM),
        ],
        out_specs=(pl.BlockSpec(memory_space=pltpu.VMEM),) * 2,
        scratch_shapes=stages((NCH,), (part, KW))
        + [vm(NCH, 2, 2, 2, part, KW)]
        + [
            vm(4, 6, 16, PW), vm(4, 6, 16, PW), vm(3, 6, 16, PW), vm(6, 16, PW), vm(3, 6, 16, PW),
            vm(2, 4, 4, 6, 16, PW),
            vm(NK, 8, 16, cols),
            pltpu.VMEM(panel_inverse.shape, F32),
            vm((NK - 1) * PW, (NK - 1) * PW),
            vm(KW, KW),
            pltpu.SemaphoreType.DMA((copies,)),
            pltpu.SemaphoreType.DMA((copies,)),
            pltpu.SemaphoreType.DMA((3,)),
        ],
        compiler_params=pltpu.CompilerParams(
            collective_id=0, has_side_effects=True, vmem_limit_bytes=28 << 20
        ),
    )(
        panel_index, raw, cross,
        pltpu.with_memory_space_constraint(factor_rows, pltpu.HBM),
        pltpu.with_memory_space_constraint(panel_inverse, pltpu.HBM),
    )
    return err.reshape(-1, KW), fac.reshape(KW, cols)


def apply_kernel(index_ref, w_ref, e_ref, f_ref, o_ref):
    cols = w_ref.shape[1]
    ids = lax.broadcasted_iota(jnp.int32, (1, cols), 1) + lax.axis_index("col") * cols
    removed = jnp.zeros((1, cols), jnp.bool_)
    for k in range(NK + 1):
        start = index_ref[k] * PW
        removed = jnp.logical_or(removed, jnp.logical_and(ids >= start, ids < start + PW))
    update = jnp.dot(e_ref[...], f_ref[...], preferred_element_type=F32)
    o_ref[...] = jnp.where(removed, 0.0, w_ref[...] - update)


def apply(panel_index, weights, err, fac):
    rows, cols = weights.shape
    tile = 128
    return pl.pallas_call(
        apply_kernel,
        out_shape=jax.ShapeDtypeStruct((rows, cols), F32),
        grid=(rows // tile,),
        in_specs=[
            pl.BlockSpec(memory_space=pltpu.SMEM),
            pl.BlockSpec((tile, cols), lambda i: (i, 0)),
            pl.BlockSpec((tile, KW), lambda i: (i, 0)),
            pl.BlockSpec(memory_space=pltpu.VMEM),
        ],
        out_specs=pl.BlockSpec((tile, cols), lambda i: (i, 0)),
        compiler_params=pltpu.CompilerParams(vmem_limit_bytes=24 << 20),
    )(panel_index, weights, err, fac)


def local(weights, factor_rows, panel_inverse, panel_index):
    hbm = lambda v: pltpu.with_memory_space_constraint(v, pltpu.HBM)
    raw, cross = extract(panel_index, hbm(weights), hbm(factor_rows))
    err, fac = exchange(panel_index, raw, cross, factor_rows, panel_inverse)
    return apply(panel_index, weights, err, fac)


def solution(mesh):
    placed = (P("row", "col"), P(None, "row", "col"), P(), P())
    return jax.shard_map(
        local, mesh=mesh, in_specs=placed, out_specs=P("row", "col"), check_vma=False
    )
```

```python
import functools

import jax
import jax.numpy as jnp
from jax import lax
from jax.experimental import pallas as pl
from jax.experimental.pallas import tpu as pltpu
from jax.sharding import PartitionSpec as P

MESH = pl.DeviceIdType.MESH
BF16 = jnp.bfloat16
F32 = jnp.float32
PW = 128
NK = 7
KW = NK * PW
NCH = 3
TILES = 24
PAIRS = [(j, k) for k in range(1, NK) for j in range(k)]


def extract_kernel(index_ref, w_ref, f_ref, raw_ref, cross_ref, wbuf, fbuf, wsem, fsem):
    cols = w_ref.shape[1]
    here = lax.axis_index("col") * cols

    def copies(k):
        first = pl.multiple_of(index_ref[k] * PW - here, PW)
        return (
            pltpu.make_async_copy(w_ref.at[:, pl.ds(first, PW)], wbuf.at[k], wsem.at[k]),
            pltpu.make_async_copy(f_ref.at[:, :, pl.ds(first, PW)], fbuf.at[k], fsem.at[k]),
        )

    def mine(k):
        first = index_ref[k] * PW - here
        return jnp.logical_and(first >= 0, first < cols)

    for k in range(NK):

        @pl.when(mine(k))
        def _():
            for copy in copies(k):
                copy.start()

    cross_ref[...] = jnp.zeros_like(cross_ref)
    for k in range(NK):

        @pl.when(jnp.logical_not(mine(k)))
        def _():
            raw_ref[:, k * PW : (k + 1) * PW] = jnp.zeros((raw_ref.shape[0], PW), BF16)

    for k in range(NK):

        @pl.when(mine(k))
        def _():
            for copy in copies(k):
                copy.wait()
            raw_ref[:, k * PW : (k + 1) * PW] = wbuf[k].astype(BF16)
            for block, (j, kk) in enumerate(PAIRS):
                if kk == k:
                    cross_ref[block] = fbuf[k, j]


def extract(panel_index, weights, factor_rows):
    rows = weights.shape[0]
    depth = factor_rows.shape[1]
    return pl.pallas_call(
        extract_kernel,
        out_shape=(
            jax.ShapeDtypeStruct((rows, KW), BF16),
            jax.ShapeDtypeStruct((TILES, depth, PW), BF16),
        ),
        in_specs=[
            pl.BlockSpec(memory_space=pltpu.SMEM),
            pl.BlockSpec(memory_space=pltpu.HBM),
            pl.BlockSpec(memory_space=pltpu.HBM),
        ],
        out_specs=(
            pl.BlockSpec(memory_space=pltpu.VMEM),
            pl.BlockSpec(memory_space=pltpu.VMEM),
        ),
        scratch_shapes=[
            pltpu.VMEM((NK, rows, PW), F32),
            pltpu.VMEM((NK,) + factor_rows.shape[:2] + (PW,), BF16),
            pltpu.SemaphoreType.DMA((NK,)),
            pltpu.SemaphoreType.DMA((NK,)),
        ],
        compiler_params=pltpu.CompilerParams(vmem_limit_bytes=24 << 20),
    )(panel_index, weights, factor_rows)


def exchange_kernel(
    index_ref, raw_ref, cross_ref, f_ref, pinv_hbm, err_ref, masked_ref,
    a_raw, m_raw, r1_raw, acc_raw, r4_raw, s_raw, z_raw, full_raw,
    a_c, m_c, r_c, s_c, z_c, full_c,
    fac_ref, pinv_ref, cmat, comp, send_sem, recv_sem, local_sem,
):
    x = lax.axis_index("row")
    col = lax.axis_index("col")
    core = col % 2
    y = (col // 2) % 4
    z = col // 8
    f = y * (1 - core) + z * core
    s = z * (1 - core) + y * core

    def at(ff, ss):
        yy, zz = ff * (1 - core) + ss * core, ss * (1 - core) + ff * core
        return {"col": zz * 8 + yy * 2 + core}

    def flip1(v):
        return v + 1 - 2 * (v % 2)

    f1, f3, s1, s3 = flip1(f), 3 - f, flip1(s), 3 - s
    x1, x3, x2 = {"row": flip1(x)}, {"row": 3 - x}, {"row": (x + 2) % 4}
    mate = {"col": col + 1 - 2 * core}
    first_others = [at((f + d) % 4, s) for d in (1, 2, 3)]
    second_others = [at(f, (s + d) % 4) for d in (1, 2, 3)]
    k1, k2, kt = (f % 2 + f // 2) % 2, f // 2, (s % 2 + s // 2) % 2
    l1, l2, lt = f // 2, f % 2, s // 2

    barrier = pltpu.get_barrier_semaphore()
    peers = first_others + second_others + [at(f1, s3), at(f3, s1), x1, x2, x3, mate]
    for peer in peers:
        pl.semaphore_signal(barrier, inc=1, device_id=peer, device_id_type=MESH)
    pl.semaphore_wait(barrier, len(peers))

    count = [0]
    sent = []

    def send(src, dst, peer):
        slot = count[0]
        count[0] += 1
        copy = pltpu.make_async_remote_copy(
            src_ref=src, dst_ref=dst, send_sem=send_sem.at[slot], recv_sem=recv_sem.at[slot],
            device_id=peer, device_id_type=MESH,
        )
        copy.start()
        sent.append(copy)
        return copy

    def arrive(copies):
        for copy in copies:
            copy.wait_recv()

    own = [
        pltpu.make_async_copy(f_ref.at[pl.ds(0, NK), h], fac_ref.at[:, x * 2 + h], local_sem.at[h])
        for h in range(2)
    ]
    fac_waits = []

    def factors_first():
        fac_waits.append(send(f_ref.at[pl.ds(0, NK), 0], fac_ref.at[:, x * 2], x1))
        fac_waits.append(send(f_ref.at[pl.ds(0, NK), 1], fac_ref.at[:, x * 2 + 1], x3))
        for copy in own:
            copy.start()

    def factors_second():
        arrive(fac_waits)
        fac_waits.clear()
        for copy in own:
            copy.wait()
        o1, o3 = flip1(x), 3 - x
        moves = ((x * 2, x3), (x * 2 + 1, x1), (o1 * 2, x3), (o3 * 2 + 1, x1))
        for k in range(NK):
            fac_waits.append(
                [send(fac_ref.at[k, slot], fac_ref.at[k, slot], peer) for slot, peer in moves]
            )

    def cross_steps():
        copies = [send(cross_ref.at[1 - core], a_c, mate)]
        yield
        arrive(copies)
        m_c[...] = cross_ref[core] + a_c[...]
        copies = [
            send(m_c.at[(f + d) % 4], r_c.at[d - 1], first_others[d - 1]) for d in (1, 2, 3)
        ]
        yield
        arrive(copies)
        s_c[...] = m_c[f] + r_c[0] + r_c[1] + r_c[2]
        copies = [send(s_c, z_c.at[d], second_others[d]) for d in range(3)]
        yield
        arrive(copies)
        mine = full_c.at[core, f]
        mine[x] = s_c[...] + z_c[0] + z_c[1] + z_c[2]
        copies = [send(mine.at[x], mine.at[x], peer) for peer in (x1, x3, x2)]
        yield
        arrive(copies)
        copies = [send(mine, mine, peer) for peer in first_others]
        yield
        arrive(copies)
        copies = [send(full_c.at[core], full_c.at[core], mate)]
        yield
        arrive(copies)
        compose()

    def compose():
        for block, (j, k) in enumerate(PAIRS):
            owner, within = block // 12, block % 12
            for half in range(2):
                tile = within * 2 + half
                for t in range(4):
                    row = j * PW + t * 32 + half * 16
                    cmat[row : row + 16, (k - 1) * PW : k * PW] = full_c[owner, tile // 6, t, tile % 6]
        pinv_copy.wait()
        comp[...] = jnp.zeros_like(comp)
        for k in range(NK):
            cols = slice(k * PW, (k + 1) * PW)
            comp[cols, cols] = pinv_ref[k].astype(BF16)
            if k:
                top = k * PW
                carried = jnp.dot(
                    comp[:top, :top], cmat[:top, (k - 1) * PW : k * PW], preferred_element_type=F32
                )
                comp[:top, cols] = (
                    -jnp.dot(
                        carried, pinv_ref[k], precision=lax.Precision.HIGHEST, preferred_element_type=F32
                    )
                ).astype(BF16)

    def chunk_steps(c):
        m, r1, acc, r4 = m_raw.at[c], r1_raw.at[c], acc_raw.at[c], r4_raw.at[c]
        sm, zr, full = s_raw.at[c], z_raw.at[c], full_raw.at[c]
        copies = [send(raw_ref.at[c, 1 - core], a_raw.at[c], mate)]
        yield
        arrive(copies)
        m[...] = raw_ref[c, core] + a_raw[c]
        copies = [
            send(m.at[0, 1 - k1], r1.at[0], at(f1, s)),
            send(m.at[1, 1 - l1], r1.at[1], at(f3, s)),
        ]
        yield
        arrive(copies)
        acc[0] = m[0, k1] + r1[0]
        acc[1] = m[1, l1] + r1[1]
        copies = [
            send(acc.at[0, 1 - k2, 1 - kt], r4.at[0, 2], at(f3, s1)),
            send(acc.at[1, 1 - l2, 1 - lt], r4.at[1, 2], at(f1, s3)),
            send(acc.at[0, 1 - k2, kt], r4.at[0, 0], at(f3, s)),
            send(acc.at[0, k2, 1 - kt], r4.at[0, 1], at(f, s1)),
            send(acc.at[1, 1 - l2, lt], r4.at[1, 0], at(f1, s)),
            send(acc.at[1, l2, 1 - lt], r4.at[1, 1], at(f, s3)),
        ]
        yield
        arrive(copies)
        sm[0] = acc[0, k2, kt] + r4[0, 0] + r4[0, 1] + r4[0, 2]
        sm[1] = acc[1, l2, lt] + r4[1, 0] + r4[1, 1] + r4[1, 2]
        copies = [send(sm.at[0], zr.at[0], at(f, s3)), send(sm.at[1], zr.at[1], at(f, s1))]
        yield
        arrive(copies)
        full[0, k1, k2, kt] = sm[0] + zr[0]
        full[1, l1, l2, lt] = sm[1] + zr[1]
        piece0, piece1 = full.at[0, k1, k2, kt], full.at[1, l1, l2, lt]
        copies = [
            send(piece, piece, peer)
            for piece, peer in (
                (piece0, at(f3, s1)), (piece1, at(f1, s3)), (piece0, at(f3, s)),
                (piece0, at(f, s1)), (piece1, at(f1, s)), (piece1, at(f, s3)),
            )
        ]
        yield
        arrive(copies)
        copies = [
            send(full.at[0, k1], full.at[0, k1], at(f1, s)),
            send(full.at[1, l1], full.at[1, l1], at(f3, s)),
        ]
        yield
        arrive(copies)
        rows = err_ref.shape[2]
        panel_cols = full[...].reshape(rows, KW)
        for lo in range(0, KW, 2 * PW):
            hi = min(lo + 2 * PW, KW)
            err_ref[c, core, :, lo:hi] = jnp.dot(
                panel_cols[:, :hi], comp[:hi, lo:hi], preferred_element_type=F32
            ).astype(BF16)
        copies = [send(err_ref.at[c, core], err_ref.at[c, core], mate)]
        yield
        arrive(copies)

    def mask_factors():
        cols = fac_ref.shape[3]
        ids = lax.broadcasted_iota(jnp.int32, (16, cols), 1) + col * cols
        for k in range(NK):
            arrive(fac_waits[k])
            keep = jnp.where(ids >= index_ref[k] * PW + PW, 1.0, 0.0).astype(BF16)
            for part in range(8):
                masked_ref[k, part] = fac_ref[k, part] * keep

    pinv_copy = pltpu.make_async_copy(pinv_hbm, pinv_ref, local_sem.at[2])
    pinv_copy.start()
    factors_first()
    cross = cross_steps()
    chunks = [chunk_steps(c) for c in range(NCH)]
    for tick in range(6):
        for flow in [cross] + chunks:
            next(flow)
        if tick == 3:
            factors_second()
    next(cross, None)
    for flow in chunks:
        next(flow)
    mask_factors()
    for flow in chunks:
        next(flow, None)
    for copy in sent:
        copy.wait_send()


def exchange(panel_index, raw, cross, factor_rows, panel_inverse):
    cols = factor_rows.shape[2]
    piece = raw.shape[0] // (NCH * 32)
    raw = raw.reshape(NCH, 2, 2, 2, 2, 2, piece, KW)
    cross = cross.reshape(2, 4, 6, 16, PW)
    factor_rows = factor_rows.reshape(8, 2, 16, cols)
    vm = lambda *shape: pltpu.VMEM(shape, BF16)
    rows = lambda *inner: vm(NCH, 2, *inner, piece, KW)
    copies = 2 + NK * 4 + NCH * 20 + 14
    err, fac = pl.pallas_call(
        exchange_kernel,
        out_shape=(
            jax.ShapeDtypeStruct((NCH, 2, 16 * piece, KW), BF16),
            jax.ShapeDtypeStruct((NK, 8, 16, cols), BF16),
        ),
        in_specs=[
            pl.BlockSpec(memory_space=pltpu.SMEM),
            pl.BlockSpec(memory_space=pltpu.VMEM),
            pl.BlockSpec(memory_space=pltpu.VMEM),
            pl.BlockSpec(memory_space=pltpu.HBM),
            pl.BlockSpec(memory_space=pltpu.HBM),
        ],
        out_specs=(pl.BlockSpec(memory_space=pltpu.VMEM),) * 2,
        scratch_shapes=[
            rows(2, 2, 2), rows(2, 2, 2), rows(2, 2), rows(2, 2), rows(3), rows(), rows(),
            rows(2, 2, 2),
            vm(4, 6, 16, PW), vm(4, 6, 16, PW), vm(3, 6, 16, PW), vm(6, 16, PW), vm(3, 6, 16, PW),
            vm(2, 4, 4, 6, 16, PW),
            vm(NK, 8, 16, cols),
            pltpu.VMEM(panel_inverse.shape, F32),
            vm((NK - 1) * PW, (NK - 1) * PW),
            vm(KW, KW),
            pltpu.SemaphoreType.DMA((copies,)),
            pltpu.SemaphoreType.DMA((copies,)),
            pltpu.SemaphoreType.DMA((3,)),
        ],
        compiler_params=pltpu.CompilerParams(
            collective_id=0, has_side_effects=True, vmem_limit_bytes=28 << 20
        ),
    )(
        panel_index, raw, cross,
        pltpu.with_memory_space_constraint(factor_rows, pltpu.HBM),
        pltpu.with_memory_space_constraint(panel_inverse, pltpu.HBM),
    )
    return err.reshape(-1, KW), fac.reshape(KW, cols)


def apply_kernel(index_ref, w_ref, e_ref, f_ref, o_hbm, out, sem):
    rows, cols = w_ref.shape
    tile = 256
    here = lax.axis_index("col") * cols
    copies = []
    for n, lo in enumerate(range(0, cols, tile)):
        span = slice(lo, lo + tile)
        ids = lax.broadcasted_iota(jnp.int32, (1, tile), 1) + (here + lo)
        removed = jnp.zeros((1, tile), jnp.bool_)
        for k in range(NK + 1):
            start = index_ref[k] * PW
            removed = jnp.logical_or(removed, jnp.logical_and(ids >= start, ids < start + PW))
        for top in range(0, rows, tile):
            block = slice(top, top + tile)
            update = jnp.dot(e_ref[block], f_ref[:, span], preferred_element_type=F32)
            out[block, span] = jnp.where(removed, 0.0, w_ref[block, span] - update)
        copy = pltpu.make_async_copy(out.at[:, span], o_hbm.at[:, span], sem.at[n])
        copy.start()
        copies.append(copy)
    for copy in copies:
        copy.wait()


def apply(panel_index, weights, err, fac):
    rows, cols = weights.shape
    whole = pl.BlockSpec(memory_space=pltpu.VMEM)
    return pl.pallas_call(
        apply_kernel,
        out_shape=jax.ShapeDtypeStruct((rows, cols), F32),
        in_specs=[pl.BlockSpec(memory_space=pltpu.SMEM), whole, whole, whole],
        out_specs=pl.BlockSpec(memory_space=pltpu.HBM),
        scratch_shapes=[pltpu.VMEM((rows, cols), F32), pltpu.SemaphoreType.DMA((cols // 256,))],
        compiler_params=pltpu.CompilerParams(vmem_limit_bytes=24 << 20),
    )(panel_index, weights, err, fac)


def local(weights, factor_rows, panel_inverse, panel_index):
    hbm = lambda v: pltpu.with_memory_space_constraint(v, pltpu.HBM)
    raw, cross = extract(panel_index, hbm(weights), hbm(factor_rows))
    err, fac = exchange(panel_index, raw, cross, factor_rows, panel_inverse)
    return apply(panel_index, weights, err, fac)


def solution(mesh):
    placed = (P("row", "col"), P(None, "row", "col"), P(), P())
    return jax.shard_map(
        local, mesh=mesh, in_specs=placed, out_specs=P("row", "col"), check_vma=False
    )
```

```python
import functools

import jax
import jax.numpy as jnp
from jax import lax
from jax.experimental import pallas as pl
from jax.experimental.pallas import tpu as pltpu
from jax.sharding import PartitionSpec as P

MESH = pl.DeviceIdType.MESH
BF16 = jnp.bfloat16
F32 = jnp.float32
PW = 128
NK = 7
KW = NK * PW
NCH = 3
TILES = 24
PAIRS = [(j, k) for k in range(1, NK) for j in range(k)]


def extract_kernel(index_ref, w_ref, f_ref, raw_ref, cross_ref, wbuf, fbuf, wsem, fsem):
    cols = w_ref.shape[1]
    here = lax.axis_index("col") * cols

    def copies(k):
        first = pl.multiple_of(index_ref[k] * PW - here, PW)
        return (
            pltpu.make_async_copy(w_ref.at[:, pl.ds(first, PW)], wbuf.at[k], wsem.at[k]),
            pltpu.make_async_copy(f_ref.at[:, :, pl.ds(first, PW)], fbuf.at[k], fsem.at[k]),
        )

    def mine(k):
        first = index_ref[k] * PW - here
        return jnp.logical_and(first >= 0, first < cols)

    for k in range(NK):

        @pl.when(mine(k))
        def _():
            for copy in copies(k):
                copy.start()

    cross_ref[...] = jnp.zeros_like(cross_ref)
    for k in range(NK):

        @pl.when(jnp.logical_not(mine(k)))
        def _():
            raw_ref[:, k * PW : (k + 1) * PW] = jnp.zeros((raw_ref.shape[0], PW), BF16)

    for k in range(NK):

        @pl.when(mine(k))
        def _():
            for copy in copies(k):
                copy.wait()
            raw_ref[:, k * PW : (k + 1) * PW] = wbuf[k].astype(BF16)
            for block, (j, kk) in enumerate(PAIRS):
                if kk == k:
                    cross_ref[block] = fbuf[k, j]


def extract(panel_index, weights, factor_rows):
    rows = weights.shape[0]
    depth = factor_rows.shape[1]
    return pl.pallas_call(
        extract_kernel,
        out_shape=(
            jax.ShapeDtypeStruct((rows, KW), BF16),
            jax.ShapeDtypeStruct((TILES, depth, PW), BF16),
        ),
        in_specs=[
            pl.BlockSpec(memory_space=pltpu.SMEM),
            pl.BlockSpec(memory_space=pltpu.HBM),
            pl.BlockSpec(memory_space=pltpu.HBM),
        ],
        out_specs=(
            pl.BlockSpec(memory_space=pltpu.VMEM),
            pl.BlockSpec(memory_space=pltpu.VMEM),
        ),
        scratch_shapes=[
            pltpu.VMEM((NK, rows, PW), F32),
            pltpu.VMEM((NK,) + factor_rows.shape[:2] + (PW,), BF16),
            pltpu.SemaphoreType.DMA((NK,)),
            pltpu.SemaphoreType.DMA((NK,)),
        ],
        compiler_params=pltpu.CompilerParams(vmem_limit_bytes=24 << 20),
    )(panel_index, weights, factor_rows)


def removed_columns(index_ref, first, count):
    ids = lax.broadcasted_iota(jnp.int32, (1, count), 1) + first
    removed = jnp.zeros((1, count), jnp.bool_)
    for k in range(NK + 1):
        start = index_ref[k] * PW
        removed = jnp.logical_or(removed, jnp.logical_and(ids >= start, ids < start + PW))
    return removed


def exchange_kernel(
    index_ref, raw_ref, cross_ref, w_hbm, f_hbm, pinv_hbm,
    err_ref, masked_ref, done_ref, w0_ref, w1_ref, w2_ref, f_ref,
    a_raw, m_raw, r1_raw, acc_raw, r4_raw, s_raw, z_raw, full_raw,
    a_c, m_c, r_c, s_c, z_c, full_c,
    fac_ref, pinv_ref, cmat, comp, send_sem, recv_sem, local_sem,
):
    x = lax.axis_index("row")
    col = lax.axis_index("col")
    core = col % 2
    y = (col // 2) % 4
    z = col // 8
    f = y * (1 - core) + z * core
    s = z * (1 - core) + y * core

    def at(ff, ss):
        yy, zz = ff * (1 - core) + ss * core, ss * (1 - core) + ff * core
        return {"col": zz * 8 + yy * 2 + core}

    def flip1(v):
        return v + 1 - 2 * (v % 2)

    f1, f3, s1, s3 = flip1(f), 3 - f, flip1(s), 3 - s
    x1, x3, x2 = {"row": flip1(x)}, {"row": 3 - x}, {"row": (x + 2) % 4}
    mate = {"col": col + 1 - 2 * core}
    first_others = [at((f + d) % 4, s) for d in (1, 2, 3)]
    second_others = [at(f, (s + d) % 4) for d in (1, 2, 3)]
    k1, k2, kt = (f % 2 + f // 2) % 2, f // 2, (s % 2 + s // 2) % 2
    l1, l2, lt = f // 2, f % 2, s // 2

    w_refs = (w0_ref, w1_ref, w2_ref)
    band = w0_ref.shape[0]
    w_copies = [
        pltpu.make_async_copy(w_hbm.at[c * band : (c + 1) * band], w_refs[c], local_sem.at[c])
        for c in range(NCH)
    ]
    f_copy = pltpu.make_async_copy(f_hbm.at[pl.ds(0, NK)], f_ref, local_sem.at[NCH])
    f_copy.start()
    for copy in w_copies:
        copy.start()

    barrier = pltpu.get_barrier_semaphore()
    peers = first_others + second_others + [at(f1, s3), at(f3, s1), x1, x2, x3, mate]
    for peer in peers:
        pl.semaphore_signal(barrier, inc=1, device_id=peer, device_id_type=MESH)

    width = w0_ref.shape[1]
    pl.semaphore_wait(barrier, len(peers))

    count = [0]
    sent = []

    def send(src, dst, peer):
        slot = count[0]
        count[0] += 1
        copy = pltpu.make_async_remote_copy(
            src_ref=src, dst_ref=dst, send_sem=send_sem.at[slot], recv_sem=recv_sem.at[slot],
            device_id=peer, device_id_type=MESH,
        )
        copy.start()
        sent.append(copy)
        return copy

    def arrive(copies):
        for copy in copies:
            copy.wait_recv()

    own = [
        pltpu.make_async_copy(f_ref.at[:, h], fac_ref.at[:, x * 2 + h], local_sem.at[NCH + 1 + h])
        for h in range(2)
    ]
    fac_waits = []

    def factors_first():
        f_copy.wait()
        fac_waits.append(send(f_ref.at[:, 0], fac_ref.at[:, x * 2], x1))
        fac_waits.append(send(f_ref.at[:, 1], fac_ref.at[:, x * 2 + 1], x3))
        for copy in own:
            copy.start()

    def factors_second():
        arrive(fac_waits)
        fac_waits.clear()
        for copy in own:
            copy.wait()
        o1, o3 = flip1(x), 3 - x
        moves = ((x * 2, x3), (x * 2 + 1, x1), (o1 * 2, x3), (o3 * 2 + 1, x1))
        for k in range(NK):
            fac_waits.append(
                [send(fac_ref.at[k, slot], fac_ref.at[k, slot], peer) for slot, peer in moves]
            )

    def cross_steps():
        copies = [send(cross_ref.at[1 - core], a_c, mate)]
        yield
        arrive(copies)
        m_c[...] = cross_ref[core] + a_c[...]
        copies = [
            send(m_c.at[(f + d) % 4], r_c.at[d - 1], first_others[d - 1]) for d in (1, 2, 3)
        ]
        yield
        arrive(copies)
        s_c[...] = m_c[f] + r_c[0] + r_c[1] + r_c[2]
        copies = [send(s_c, z_c.at[d], second_others[d]) for d in range(3)]
        yield
        arrive(copies)
        mine = full_c.at[core, f]
        mine[x] = s_c[...] + z_c[0] + z_c[1] + z_c[2]
        copies = [send(mine.at[x], mine.at[x], peer) for peer in (x1, x3, x2)]
        yield
        arrive(copies)
        copies = [send(mine, mine, peer) for peer in first_others]
        yield
        arrive(copies)
        copies = [send(full_c.at[core], full_c.at[core], mate)]
        yield
        arrive(copies)
        compose()

    def compose():
        for block, (j, k) in enumerate(PAIRS):
            owner, within = block // 12, block % 12
            for half in range(2):
                tile = within * 2 + half
                for t in range(4):
                    row = j * PW + t * 32 + half * 16
                    cmat[row : row + 16, (k - 1) * PW : k * PW] = full_c[owner, tile // 6, t, tile % 6]
        pinv_copy.wait()
        comp[...] = jnp.zeros_like(comp)
        for k in range(NK):
            cols = slice(k * PW, (k + 1) * PW)
            comp[cols, cols] = pinv_ref[k].astype(BF16)
            if k:
                top = k * PW
                carried = jnp.dot(
                    comp[:top, :top], cmat[:top, (k - 1) * PW : k * PW], preferred_element_type=F32
                )
                comp[:top, cols] = (
                    -jnp.dot(
                        carried, pinv_ref[k], precision=lax.Precision.HIGHEST, preferred_element_type=F32
                    )
                ).astype(BF16)

    def chunk_steps(c):
        m, r1, acc, r4 = m_raw.at[c], r1_raw.at[c], acc_raw.at[c], r4_raw.at[c]
        sm, zr, full = s_raw.at[c], z_raw.at[c], full_raw.at[c]
        copies = [send(raw_ref.at[c, 1 - core], a_raw.at[c], mate)]
        yield
        arrive(copies)
        m[...] = raw_ref[c, core] + a_raw[c]
        copies = [
            send(m.at[0, 1 - k1], r1.at[0], at(f1, s)),
            send(m.at[1, 1 - l1], r1.at[1], at(f3, s)),
        ]
        yield
        arrive(copies)
        acc[0] = m[0, k1] + r1[0]
        acc[1] = m[1, l1] + r1[1]
        copies = [
            send(acc.at[0, 1 - k2, 1 - kt], r4.at[0, 2], at(f3, s1)),
            send(acc.at[1, 1 - l2, 1 - lt], r4.at[1, 2], at(f1, s3)),
            send(acc.at[0, 1 - k2, kt], r4.at[0, 0], at(f3, s)),
            send(acc.at[0, k2, 1 - kt], r4.at[0, 1], at(f, s1)),
            send(acc.at[1, 1 - l2, lt], r4.at[1, 0], at(f1, s)),
            send(acc.at[1, l2, 1 - lt], r4.at[1, 1], at(f, s3)),
        ]
        yield
        arrive(copies)
        sm[0] = acc[0, k2, kt] + r4[0, 0] + r4[0, 1] + r4[0, 2]
        sm[1] = acc[1, l2, lt] + r4[1, 0] + r4[1, 1] + r4[1, 2]
        copies = [send(sm.at[0], zr.at[0], at(f, s3)), send(sm.at[1], zr.at[1], at(f, s1))]
        yield
        arrive(copies)
        full[0, k1, k2, kt] = sm[0] + zr[0]
        full[1, l1, l2, lt] = sm[1] + zr[1]
        piece0, piece1 = full.at[0, k1, k2, kt], full.at[1, l1, l2, lt]
        copies = [
            send(piece, piece, peer)
            for piece, peer in (
                (piece0, at(f3, s1)), (piece1, at(f1, s3)), (piece0, at(f3, s)),
                (piece0, at(f, s1)), (piece1, at(f1, s)), (piece1, at(f, s3)),
            )
        ]
        yield
        arrive(copies)
        copies = [
            send(full.at[0, k1], full.at[0, k1], at(f1, s)),
            send(full.at[1, l1], full.at[1, l1], at(f3, s)),
        ]
        yield
        arrive(copies)
        rows = err_ref.shape[2]
        panel_cols = full[...].reshape(rows, KW)
        for lo in range(0, KW, 2 * PW):
            hi = min(lo + 2 * PW, KW)
            err_ref[c, core, :, lo:hi] = jnp.dot(
                panel_cols[:, :hi], comp[:hi, lo:hi], preferred_element_type=F32
            ).astype(BF16)
        copies = [send(err_ref.at[c, core], err_ref.at[c, core], mate)]
        yield
        arrive(copies)

    def mask_factors():
        cols = fac_ref.shape[3]
        ids = lax.broadcasted_iota(jnp.int32, (16, cols), 1) + col * cols
        for k in range(NK):
            arrive(fac_waits[k])
            keep = jnp.where(ids >= index_ref[k] * PW + PW, 1.0, 0.0).astype(BF16)
            for part in range(8):
                masked_ref[k, part] = fac_ref[k, part] * keep

    pinv_copy = pltpu.make_async_copy(pinv_hbm, pinv_ref, local_sem.at[NCH + 3])
    def own_block(c):
        w_copies[c].wait()
        rows, tile = err_ref.shape[2], 2 * PW
        for lo in range(0, width, tile):
            span = slice(lo, lo + tile)
            factors = masked_ref[:, :, :, span].reshape(KW, tile)
            update = jnp.dot(err_ref[c, core], factors, preferred_element_type=F32)
            before = w_refs[c][pl.ds(pl.multiple_of(core * rows, rows), rows), span]
            removed = removed_columns(index_ref, col * width + lo, tile)
            done_ref[c, :, span] = jnp.where(removed, 0.0, before - update)

    pinv_copy.start()
    cross = cross_steps()
    chunks = [chunk_steps(c) for c in range(NCH)]
    for tick in range(6):
        for flow in [cross] + chunks:
            next(flow)
            if tick == 0 and flow is chunks[0]:
                factors_first()
            if tick == 3 and flow is cross:
                factors_second()
    next(cross, None)
    for flow in chunks:
        next(flow)
    mask_factors()
    for c in range(NCH):
        own_block(c)
    for flow in chunks:
        next(flow, None)
    for copy in sent:
        copy.wait_send()


def exchange(panel_index, raw, cross, weights, factor_rows, panel_inverse):
    cols = factor_rows.shape[2]
    piece = weights.shape[0] // (NCH * 32)
    band = jax.ShapeDtypeStruct((weights.shape[0] // NCH, cols), F32)
    raw = raw.reshape(NCH, 2, 2, 2, 2, 2, piece, KW)
    cross = cross.reshape(2, 4, 6, 16, PW)
    factor_rows = factor_rows.reshape(8, 2, 16, cols)
    vm = lambda *shape: pltpu.VMEM(shape, BF16)
    rows = lambda *inner: vm(NCH, 2, *inner, piece, KW)
    copies = 2 + NK * 4 + NCH * 20 + 14
    err, fac, done, *bands = pl.pallas_call(
        exchange_kernel,
        out_shape=(
            jax.ShapeDtypeStruct((NCH, 2, 16 * piece, KW), BF16),
            jax.ShapeDtypeStruct((NK, 8, 16, cols), BF16),
            jax.ShapeDtypeStruct((NCH, 16 * piece, cols), F32),
            band, band, band,
        ),
        in_specs=[
            pl.BlockSpec(memory_space=pltpu.SMEM),
            pl.BlockSpec(memory_space=pltpu.VMEM),
            pl.BlockSpec(memory_space=pltpu.VMEM),
            pl.BlockSpec(memory_space=pltpu.HBM),
            pl.BlockSpec(memory_space=pltpu.HBM),
            pl.BlockSpec(memory_space=pltpu.HBM),
        ],
        out_specs=(pl.BlockSpec(memory_space=pltpu.VMEM),) * 6,
        scratch_shapes=[
            vm(NK, 2, 16, cols),
            rows(2, 2, 2), rows(2, 2, 2), rows(2, 2), rows(2, 2), rows(3), rows(), rows(),
            rows(2, 2, 2),
            vm(4, 6, 16, PW), vm(4, 6, 16, PW), vm(3, 6, 16, PW), vm(6, 16, PW), vm(3, 6, 16, PW),
            vm(2, 4, 4, 6, 16, PW),
            vm(NK, 8, 16, cols),
            pltpu.VMEM(panel_inverse.shape, F32),
            vm((NK - 1) * PW, (NK - 1) * PW),
            vm(KW, KW),
            pltpu.SemaphoreType.DMA((copies,)),
            pltpu.SemaphoreType.DMA((copies,)),
            pltpu.SemaphoreType.DMA((NCH + 4,)),
        ],
        compiler_params=pltpu.CompilerParams(
            collective_id=0, has_side_effects=True, vmem_limit_bytes=28 << 20
        ),
    )(
        panel_index, raw, cross,
        pltpu.with_memory_space_constraint(weights, pltpu.HBM),
        pltpu.with_memory_space_constraint(factor_rows, pltpu.HBM),
        pltpu.with_memory_space_constraint(panel_inverse, pltpu.HBM),
    )
    return err, fac.reshape(KW, cols), done, bands


def apply_kernel(
    index_ref, w0_ref, w1_ref, w2_ref, e_ref, f_ref, done_ref, o_hbm, out, sem
):
    bands, rows, cols = out.shape
    tile = 256
    col = lax.axis_index("col")
    core = col % 2
    copies = []

    def send(src, band, half, span):
        top = pl.multiple_of(band * 2 * rows + half * rows, rows)
        copy = pltpu.make_async_copy(src, o_hbm.at[pl.ds(top, rows), span], sem.at[len(copies)])
        copy.start()
        copies.append(copy)

    for band in range(bands):
        send(done_ref.at[band], band, core, slice(0, cols))
    inner = pl.ds(pl.multiple_of((1 - core) * rows, rows), rows)
    for lo in range(0, cols, tile):
        span = slice(lo, lo + tile)
        removed = removed_columns(index_ref, col * cols + lo, tile)
        for band, w_ref in enumerate((w0_ref, w1_ref, w2_ref)):
            update = jnp.dot(e_ref[band, 1 - core], f_ref[:, span], preferred_element_type=F32)
            out[band, :, span] = jnp.where(removed, 0.0, w_ref[inner, span] - update)
            send(out.at[band, :, span], band, 1 - core, span)
    for copy in copies:
        copy.wait()


def apply(panel_index, bands, err, fac, done):
    cols = fac.shape[1]
    whole = pl.BlockSpec(memory_space=pltpu.VMEM)
    return pl.pallas_call(
        apply_kernel,
        out_shape=jax.ShapeDtypeStruct((NCH * 2 * done.shape[1], cols), F32),
        in_specs=[pl.BlockSpec(memory_space=pltpu.SMEM)] + [whole] * 6,
        out_specs=pl.BlockSpec(memory_space=pltpu.HBM),
        scratch_shapes=[
            pltpu.VMEM(done.shape, F32),
            pltpu.SemaphoreType.DMA((NCH + NCH * (cols // 256),)),
        ],
        compiler_params=pltpu.CompilerParams(vmem_limit_bytes=16 << 20),
    )(panel_index, *bands, err, fac, done)


def local(weights, factor_rows, panel_inverse, panel_index):
    hbm = lambda v: pltpu.with_memory_space_constraint(v, pltpu.HBM)
    raw, cross = extract(panel_index, hbm(weights), hbm(factor_rows))
    err, fac, done, bands = exchange(panel_index, raw, cross, weights, factor_rows, panel_inverse)
    return apply(panel_index, bands, err, fac, done)


def solution(mesh):
    placed = (P("row", "col"), P(None, "row", "col"), P(), P())
    return jax.shard_map(
        local, mesh=mesh, in_specs=placed, out_specs=P("row", "col"), check_vma=False
    )
```

```python
import functools

import jax
import jax.numpy as jnp
from jax import lax
from jax.experimental import pallas as pl
from jax.experimental.pallas import tpu as pltpu
from jax.sharding import PartitionSpec as P

MESH = pl.DeviceIdType.MESH
BF16 = jnp.bfloat16
F32 = jnp.float32
PW = 128
NK = 7
KW = NK * PW
NCH = 3
TILES = 24
PAIRS = [(j, k) for k in range(1, NK) for j in range(k)]


def extract_kernel(
    index_hbm, w_ref, f_ref, raw_ref, cross_ref, index_ref, wbuf, fbuf, isem, wsem, fsem
):
    cols = w_ref.shape[1]
    here = lax.axis_index("col") * cols

    def copies(k):
        first = pl.multiple_of(index_ref[k] * PW - here, PW)
        return (
            pltpu.make_async_copy(w_ref.at[:, pl.ds(first, PW)], wbuf.at[k], wsem.at[k]),
            pltpu.make_async_copy(f_ref.at[:, :, pl.ds(first, PW)], fbuf.at[k], fsem.at[k]),
        )

    def mine(k):
        first = index_ref[k] * PW - here
        return jnp.logical_and(first >= 0, first < cols)

    index_copy = pltpu.make_async_copy(index_hbm, index_ref, isem)
    index_copy.start()
    cross_ref[...] = jnp.zeros_like(cross_ref)
    raw_ref[...] = jnp.zeros_like(raw_ref)
    index_copy.wait()
    for k in range(NK):

        @pl.when(mine(k))
        def _():
            for copy in copies(k):
                copy.start()

    for k in range(NK):

        @pl.when(mine(k))
        def _():
            for copy in copies(k):
                copy.wait()
            raw_ref[:, k * PW : (k + 1) * PW] = wbuf[k].astype(BF16)
            for block, (j, kk) in enumerate(PAIRS):
                if kk == k:
                    cross_ref[block] = fbuf[k, j]


def extract(panel_index, weights, factor_rows):
    rows = weights.shape[0]
    depth = factor_rows.shape[1]
    return pl.pallas_call(
        extract_kernel,
        out_shape=(
            jax.ShapeDtypeStruct((rows, KW), BF16),
            jax.ShapeDtypeStruct((TILES, depth, PW), BF16),
        ),
        in_specs=[
            pl.BlockSpec(memory_space=pltpu.HBM),
            pl.BlockSpec(memory_space=pltpu.HBM),
            pl.BlockSpec(memory_space=pltpu.HBM),
        ],
        out_specs=(
            pl.BlockSpec(memory_space=pltpu.VMEM),
            pl.BlockSpec(memory_space=pltpu.VMEM),
        ),
        scratch_shapes=[
            pltpu.SMEM(panel_index.shape, jnp.int32),
            pltpu.VMEM((NK, rows, PW), F32),
            pltpu.VMEM((NK,) + factor_rows.shape[:2] + (PW,), BF16),
            pltpu.SemaphoreType.DMA,
            pltpu.SemaphoreType.DMA((NK,)),
            pltpu.SemaphoreType.DMA((NK,)),
        ],
        compiler_params=pltpu.CompilerParams(vmem_limit_bytes=24 << 20),
    )(panel_index, weights, factor_rows)


def removed_columns(index_ref, first, count):
    ids = lax.broadcasted_iota(jnp.int32, (1, count), 1) + first
    removed = jnp.zeros((1, count), jnp.bool_)
    for k in range(NK + 1):
        start = index_ref[k] * PW
        removed = jnp.logical_or(removed, jnp.logical_and(ids >= start, ids < start + PW))
    return removed


def exchange_kernel(
    index_ref, raw_ref, cross_ref, w_hbm, f_hbm, pinv_hbm,
    err_ref, masked_ref, done_ref, w0_ref, w1_ref, w2_ref, f_ref,
    a_raw, m_raw, r1_raw, acc_raw, r4_raw, s_raw, z_raw, full_raw,
    a_c, m_c, r_c, s_c, z_c, full_c,
    fac_ref, pinv_ref, cmat, comp, send_sem, recv_sem, local_sem,
):
    x = lax.axis_index("row")
    col = lax.axis_index("col")
    core = col % 2
    y = (col // 2) % 4
    z = col // 8
    f = y * (1 - core) + z * core
    s = z * (1 - core) + y * core

    def at(ff, ss):
        yy, zz = ff * (1 - core) + ss * core, ss * (1 - core) + ff * core
        return {"col": zz * 8 + yy * 2 + core}

    def flip1(v):
        return v + 1 - 2 * (v % 2)

    f1, f3, s1, s3 = flip1(f), 3 - f, flip1(s), 3 - s
    x1, x3, x2 = {"row": flip1(x)}, {"row": 3 - x}, {"row": (x + 2) % 4}
    mate = {"col": col + 1 - 2 * core}
    first_others = [at((f + d) % 4, s) for d in (1, 2, 3)]
    second_others = [at(f, (s + d) % 4) for d in (1, 2, 3)]
    k1, k2, kt = (f % 2 + f // 2) % 2, f // 2, (s % 2 + s // 2) % 2
    l1, l2, lt = f // 2, f % 2, s // 2

    w_refs = (w0_ref, w1_ref, w2_ref)
    band = w0_ref.shape[0]
    w_copies = [
        pltpu.make_async_copy(w_hbm.at[c * band : (c + 1) * band], w_refs[c], local_sem.at[c])
        for c in range(NCH)
    ]
    f_copy = pltpu.make_async_copy(f_hbm.at[pl.ds(0, NK)], f_ref, local_sem.at[NCH])
    f_copy.start()
    for copy in w_copies:
        copy.start()

    barrier = pltpu.get_barrier_semaphore()
    peers = first_others + second_others + [at(f1, s3), at(f3, s1), x1, x2, x3, mate]
    for peer in peers:
        pl.semaphore_signal(barrier, inc=1, device_id=peer, device_id_type=MESH)

    width = w0_ref.shape[1]
    pl.semaphore_wait(barrier, len(peers))

    count = [0]
    sent = []

    def send(src, dst, peer):
        slot = count[0]
        count[0] += 1
        copy = pltpu.make_async_remote_copy(
            src_ref=src, dst_ref=dst, send_sem=send_sem.at[slot], recv_sem=recv_sem.at[slot],
            device_id=peer, device_id_type=MESH,
        )
        copy.start()
        sent.append(copy)
        return copy

    def arrive(copies):
        for copy in copies:
            copy.wait_recv()

    own = [
        pltpu.make_async_copy(f_ref.at[:, h], fac_ref.at[:, x * 2 + h], local_sem.at[NCH + 1 + h])
        for h in range(2)
    ]
    fac_waits = []

    def factors_first():
        f_copy.wait()
        fac_waits.append(send(f_ref.at[:, 0], fac_ref.at[:, x * 2], x1))
        fac_waits.append(send(f_ref.at[:, 1], fac_ref.at[:, x * 2 + 1], x3))
        for copy in own:
            copy.start()

    def factors_second():
        arrive(fac_waits)
        fac_waits.clear()
        for copy in own:
            copy.wait()
        o1, o3 = flip1(x), 3 - x
        moves = ((x * 2, x3), (x * 2 + 1, x1), (o1 * 2, x3), (o3 * 2 + 1, x1))
        for k in range(NK):
            fac_waits.append(
                [send(fac_ref.at[k, slot], fac_ref.at[k, slot], peer) for slot, peer in moves]
            )

    def cross_steps():
        copies = [send(cross_ref.at[1 - core], a_c, mate)]
        yield
        arrive(copies)
        m_c[...] = cross_ref[core] + a_c[...]
        copies = [
            send(m_c.at[(f + d) % 4], r_c.at[d - 1], first_others[d - 1]) for d in (1, 2, 3)
        ]
        yield
        arrive(copies)
        s_c[...] = m_c[f] + r_c[0] + r_c[1] + r_c[2]
        copies = [send(s_c, z_c.at[d], second_others[d]) for d in range(3)]
        yield
        arrive(copies)
        mine = full_c.at[core, f]
        mine[x] = s_c[...] + z_c[0] + z_c[1] + z_c[2]
        copies = [send(mine.at[x], mine.at[x], peer) for peer in (x1, x3, x2)]
        yield
        arrive(copies)
        copies = [send(mine, mine, peer) for peer in first_others]
        yield
        arrive(copies)
        copies = [send(full_c.at[core], full_c.at[core], mate)]
        yield
        arrive(copies)
        compose()

    def compose():
        for block, (j, k) in enumerate(PAIRS):
            owner, within = block // 12, block % 12
            for half in range(2):
                tile = within * 2 + half
                for t in range(4):
                    row = j * PW + t * 32 + half * 16
                    cmat[row : row + 16, (k - 1) * PW : k * PW] = full_c[owner, tile // 6, t, tile % 6]
        pinv_copy.wait()
        comp[...] = jnp.zeros_like(comp)
        for k in range(NK):
            cols = slice(k * PW, (k + 1) * PW)
            comp[cols, cols] = pinv_ref[k].astype(BF16)
            if k:
                top = k * PW
                carried = jnp.dot(
                    comp[:top, :top], cmat[:top, (k - 1) * PW : k * PW], preferred_element_type=F32
                )
                comp[:top, cols] = (
                    -jnp.dot(
                        carried, pinv_ref[k], precision=lax.Precision.HIGHEST, preferred_element_type=F32
                    )
                ).astype(BF16)

    def chunk_steps(c):
        m, r1, acc, r4 = m_raw.at[c], r1_raw.at[c], acc_raw.at[c], r4_raw.at[c]
        sm, zr, full = s_raw.at[c], z_raw.at[c], full_raw.at[c]
        copies = [send(raw_ref.at[c, 1 - core], a_raw.at[c], mate)]
        yield
        arrive(copies)
        m[...] = raw_ref[c, core] + a_raw[c]
        copies = [
            send(m.at[0, 1 - k1], r1.at[0], at(f1, s)),
            send(m.at[1, 1 - l1], r1.at[1], at(f3, s)),
        ]
        yield
        arrive(copies)
        acc[0] = m[0, k1] + r1[0]
        acc[1] = m[1, l1] + r1[1]
        copies = [
            send(acc.at[0, 1 - k2, 1 - kt], r4.at[0, 2], at(f3, s1)),
            send(acc.at[1, 1 - l2, 1 - lt], r4.at[1, 2], at(f1, s3)),
            send(acc.at[0, 1 - k2, kt], r4.at[0, 0], at(f3, s)),
            send(acc.at[0, k2, 1 - kt], r4.at[0, 1], at(f, s1)),
            send(acc.at[1, 1 - l2, lt], r4.at[1, 0], at(f1, s)),
            send(acc.at[1, l2, 1 - lt], r4.at[1, 1], at(f, s3)),
        ]
        yield
        arrive(copies)
        sm[0] = acc[0, k2, kt] + r4[0, 0] + r4[0, 1] + r4[0, 2]
        sm[1] = acc[1, l2, lt] + r4[1, 0] + r4[1, 1] + r4[1, 2]
        copies = [send(sm.at[0], zr.at[0], at(f, s3)), send(sm.at[1], zr.at[1], at(f, s1))]
        yield
        arrive(copies)
        full[0, k1, k2, kt] = sm[0] + zr[0]
        full[1, l1, l2, lt] = sm[1] + zr[1]
        piece0, piece1 = full.at[0, k1, k2, kt], full.at[1, l1, l2, lt]
        copies = [
            send(piece, piece, peer)
            for piece, peer in (
                (piece0, at(f3, s1)), (piece1, at(f1, s3)), (piece0, at(f3, s)),
                (piece0, at(f, s1)), (piece1, at(f1, s)), (piece1, at(f, s3)),
            )
        ]
        yield
        arrive(copies)
        copies = [
            send(full.at[0, k1], full.at[0, k1], at(f1, s)),
            send(full.at[1, l1], full.at[1, l1], at(f3, s)),
        ]
        yield
        arrive(copies)
        rows = err_ref.shape[2]
        panel_cols = full[...].reshape(rows, KW)
        for lo in range(0, KW, 2 * PW):
            hi = min(lo + 2 * PW, KW)
            err_ref[c, core, :, lo:hi] = jnp.dot(
                panel_cols[:, :hi], comp[:hi, lo:hi], preferred_element_type=F32
            ).astype(BF16)
        copies = [send(err_ref.at[c, core], err_ref.at[c, core], mate)]
        yield
        arrive(copies)

    def mask_factors():
        cols = fac_ref.shape[3]
        ids = lax.broadcasted_iota(jnp.int32, (16, cols), 1) + col * cols
        for k in range(NK):
            arrive(fac_waits[k])
            keep = jnp.where(ids >= index_ref[k] * PW + PW, 1.0, 0.0).astype(BF16)
            for part in range(8):
                masked_ref[k, part] = fac_ref[k, part] * keep

    pinv_copy = pltpu.make_async_copy(pinv_hbm, pinv_ref, local_sem.at[NCH + 3])
    def own_block(c):
        w_copies[c].wait()
        rows, tile = err_ref.shape[2], 2 * PW
        for lo in range(0, width, tile):
            span = slice(lo, lo + tile)
            factors = masked_ref[:, :, :, span].reshape(KW, tile)
            update = jnp.dot(err_ref[c, core], factors, preferred_element_type=F32)
            before = w_refs[c][pl.ds(pl.multiple_of(core * rows, rows), rows), span]
            removed = removed_columns(index_ref, col * width + lo, tile)
            done_ref[c, :, span] = jnp.where(removed, 0.0, before - update)

    pinv_copy.start()
    cross = cross_steps()
    chunks = [chunk_steps(c) for c in range(NCH)]
    for tick in range(6):
        for flow in [cross] + chunks:
            next(flow)
            if tick == 0 and flow is chunks[0]:
                factors_first()
            if tick == 3 and flow is cross:
                factors_second()
    next(cross, None)
    for flow in chunks:
        next(flow)
    mask_factors()
    for c in range(NCH):
        own_block(c)
    for flow in chunks:
        next(flow, None)
    for copy in sent:
        copy.wait_send()


def exchange(panel_index, raw, cross, weights, factor_rows, panel_inverse):
    cols = factor_rows.shape[2]
    piece = weights.shape[0] // (NCH * 32)
    band = jax.ShapeDtypeStruct((weights.shape[0] // NCH, cols), F32)
    raw = raw.reshape(NCH, 2, 2, 2, 2, 2, piece, KW)
    cross = cross.reshape(2, 4, 6, 16, PW)
    factor_rows = factor_rows.reshape(8, 2, 16, cols)
    vm = lambda *shape: pltpu.VMEM(shape, BF16)
    rows = lambda *inner: vm(NCH, 2, *inner, piece, KW)
    copies = 2 + NK * 4 + NCH * 20 + 14
    err, fac, done, *bands = pl.pallas_call(
        exchange_kernel,
        out_shape=(
            jax.ShapeDtypeStruct((NCH, 2, 16 * piece, KW), BF16),
            jax.ShapeDtypeStruct((NK, 8, 16, cols), BF16),
            jax.ShapeDtypeStruct((NCH, 16 * piece, cols), F32),
            band, band, band,
        ),
        in_specs=[
            pl.BlockSpec(memory_space=pltpu.SMEM),
            pl.BlockSpec(memory_space=pltpu.VMEM),
            pl.BlockSpec(memory_space=pltpu.VMEM),
            pl.BlockSpec(memory_space=pltpu.HBM),
            pl.BlockSpec(memory_space=pltpu.HBM),
            pl.BlockSpec(memory_space=pltpu.HBM),
        ],
        out_specs=(pl.BlockSpec(memory_space=pltpu.VMEM),) * 6,
        scratch_shapes=[
            vm(NK, 2, 16, cols),
            rows(2, 2, 2), rows(2, 2, 2), rows(2, 2), rows(2, 2), rows(3), rows(), rows(),
            rows(2, 2, 2),
            vm(4, 6, 16, PW), vm(4, 6, 16, PW), vm(3, 6, 16, PW), vm(6, 16, PW), vm(3, 6, 16, PW),
            vm(2, 4, 4, 6, 16, PW),
            vm(NK, 8, 16, cols),
            pltpu.VMEM(panel_inverse.shape, F32),
            vm((NK - 1) * PW, (NK - 1) * PW),
            vm(KW, KW),
            pltpu.SemaphoreType.DMA((copies,)),
            pltpu.SemaphoreType.DMA((copies,)),
            pltpu.SemaphoreType.DMA((NCH + 4,)),
        ],
        compiler_params=pltpu.CompilerParams(
            collective_id=0, has_side_effects=True, vmem_limit_bytes=28 << 20
        ),
    )(
        panel_index, raw, cross,
        pltpu.with_memory_space_constraint(weights, pltpu.HBM),
        pltpu.with_memory_space_constraint(factor_rows, pltpu.HBM),
        pltpu.with_memory_space_constraint(panel_inverse, pltpu.HBM),
    )
    return err, fac.reshape(KW, cols), done, bands


def apply_kernel(
    index_ref, w0_ref, w1_ref, w2_ref, e_ref, f_ref, done_ref, o_hbm, out, sem
):
    bands, rows, cols = out.shape
    tile = 256
    col = lax.axis_index("col")
    core = col % 2
    copies = []

    def send(src, band, half, span):
        top = pl.multiple_of(band * 2 * rows + half * rows, rows)
        copy = pltpu.make_async_copy(src, o_hbm.at[pl.ds(top, rows), span], sem.at[len(copies)])
        copy.start()
        copies.append(copy)

    for band in range(bands):
        send(done_ref.at[band], band, core, slice(0, cols))
    inner = pl.ds(pl.multiple_of((1 - core) * rows, rows), rows)
    for lo in range(0, cols, tile):
        span = slice(lo, lo + tile)
        removed = removed_columns(index_ref, col * cols + lo, tile)
        for band, w_ref in enumerate((w0_ref, w1_ref, w2_ref)):
            update = jnp.dot(e_ref[band, 1 - core], f_ref[:, span], preferred_element_type=F32)
            out[band, :, span] = jnp.where(removed, 0.0, w_ref[inner, span] - update)
            send(out.at[band, :, span], band, 1 - core, span)
    for copy in copies:
        copy.wait()


def apply(panel_index, bands, err, fac, done):
    cols = fac.shape[1]
    whole = pl.BlockSpec(memory_space=pltpu.VMEM)
    return pl.pallas_call(
        apply_kernel,
        out_shape=jax.ShapeDtypeStruct((NCH * 2 * done.shape[1], cols), F32),
        in_specs=[pl.BlockSpec(memory_space=pltpu.SMEM)] + [whole] * 6,
        out_specs=pl.BlockSpec(memory_space=pltpu.HBM),
        scratch_shapes=[
            pltpu.VMEM(done.shape, F32),
            pltpu.SemaphoreType.DMA((NCH + NCH * (cols // 256),)),
        ],
        compiler_params=pltpu.CompilerParams(vmem_limit_bytes=16 << 20),
    )(panel_index, *bands, err, fac, done)


def local(weights, factor_rows, panel_inverse, panel_index):
    hbm = lambda v: pltpu.with_memory_space_constraint(v, pltpu.HBM)
    raw, cross = extract(hbm(panel_index), hbm(weights), hbm(factor_rows))
    err, fac, done, bands = exchange(panel_index, raw, cross, weights, factor_rows, panel_inverse)
    return apply(panel_index, bands, err, fac, done)


def solution(mesh):
    placed = (P("row", "col"), P(None, "row", "col"), P(), P())
    return jax.shard_map(
        local, mesh=mesh, in_specs=placed, out_specs=P("row", "col"), check_vma=False
    )
```
